32 devices in a mesh: seq: 4 (over y, x), exp: 8 (over z, core).
Axes of the slice: x: 2, y: 2, z: 4, core: 2. Of those that a mesh axis runs over, the one named last changes fastest.
Arguments:
- patches: bfloat16 [4096, 2048], P(('seq', 'exp')), may hold values from -6 to 6
- routes: int32 [4096, 2], P(('seq', 'exp')), may hold values from 0 to 7, all different within a row; in each aligned block of 128 rows (0 to 127, 128 to 255, ...) at most 40 rows name the same one
- mix_weights: float32 [4096, 2], P(('seq', 'exp')), may hold values from 0.25 to 1
- modulation: float32 [2, 3, 2048], replicated, may hold values from -3 to 3
- up_weight: bfloat16 [32, 2048, 256], P(('seq', 'exp')), may hold values from -0.125 to 0.125
- down_weight: bfloat16 [32, 256, 2048], P(('seq', 'exp')), may hold values from -0.1875 to 0.1875
- cotangent: bfloat16 [4096, 2048], P(('seq', 'exp')), may hold values from -6 to 6
Outputs:
- mixed: bfloat16 [4096, 2048], P(('seq', 'exp'))
- grad_patches: bfloat16 [4096, 2048], P(('seq', 'exp'))
- grad_up: bfloat16 [32, 2048, 256], P(('seq', 'exp'))
- grad_down: bfloat16 [32, 256, 2048], P(('seq', 'exp'))
The draws below stay inside these ranges and needn't reach their ends.
Inputs may be any that keep to these rules, and one draw needn't show every extreme that they name: `routes`: in every aligned block of 128 tokens no expert is named by more than 40 assignments, a bound that some block reaches; the two experts of a token differ.
All inputs are finite; a program needn't handle non-finite values.
Results may differ from the reference program's by a relative error of at most 0.008.
Values may be sent and summed in bfloat16 or wider, within the bound.
No kernel may reach another device: no remote copies, remote signals or barrier semaphores. Data moves between devices by JAX's collectives and lax.ppermute only.
A program may use at most 128 MiB of HBM per device.

```python
import math
import jax
import jax.numpy as jnp
import numpy as np
from jax import lax

D = 2048
HIDDEN_SIZE = 1024
SPLIT = 4
LATENTS = 2
TOK_DEV = 128
TOKENS = 4096
EXPERTS = 8
CAP = 40
N_SEQ = 4
N_EXP = 8


def shard_levels(stream_key, extent, pieces, least, largest):
    def one(axis_at, blocks):
        steps = jax.random.uniform(jax.random.fold_in(jax.random.fold_in(stream_key, 6), axis_at), (blocks,), jnp.float32, least / len(pieces), largest / len(pieces))
        return jnp.repeat(jnp.exp(steps), extent[axis_at] // blocks).reshape((-1,) + (1,) * (len(extent) - axis_at - 1))

    loudness = one(*pieces[0])
    for cut in pieces[1:]:
        loudness = loudness * one(*cut)
    return loudness


def routed_block(stream_key, own, number, rows, number_of, top, reach, lean):
    ranking = jax.random.permutation(stream_key, number_of)
    heavy_load, usual = shares(number_of, rows * top, reach, lean, True), shares(number_of, rows * top, reach, lean, False)
    places = jnp.arange(number_of)

    def named(sizes, turn):
        used = int((sizes > 0).sum())
        fixed = max(1, used // 4)
        moved = fixed + (places - fixed + turn * (used - fixed)) % max(1, number_of - fixed)
        return jnp.zeros((number_of,), jnp.int32).at[ranking[jnp.where(places < fixed, places, moved)]].set(jnp.asarray(sizes, jnp.int32))

    sizes = jnp.where(number % 4 == 0, named(heavy_load, number // 4), named(usual, number - number // 4 - 1))
    mixed = jax.random.permutation(jax.random.fold_in(own, 3), number_of)
    giver, taker = mixed[0:number_of // 2 * 2:2], mixed[1:number_of // 2 * 2:2]
    slack = jnp.minimum(sizes[giver] - 1, reach - sizes[taker]) // 2
    slack = jnp.where((giver == ranking[0]) | (taker == ranking[0]) | (sizes[taker] == 0), 0, jnp.maximum(slack, 0))
    moved = jax.random.randint(jax.random.fold_in(own, 4), (number_of // 2,), 0, 1 << 20) % (slack + 1)
    sizes = sizes.at[giver].add(-moved).at[taker].add(moved)
    items = jnp.searchsorted(jnp.cumsum(sizes), jnp.arange(rows * top), side="right").astype(jnp.int32)
    listing = items.reshape(top, rows).T
    listing = listing[jax.random.permutation(jax.random.fold_in(own, 1), rows)]
    turn = jax.random.randint(jax.random.fold_in(own, 2), (rows, 1), 0, top)
    return jnp.take_along_axis(listing, (jnp.arange(top)[None, :] + turn) % top, axis=1)


def shares(number_of, total, bound, slope, full):
    weights = [(1 << 20) // math.isqrt(rank ** slope) + 1 for rank in range(1, number_of + 1)]
    largest = bound if full else min(bound, max(-(-total // number_of), total * weights[0] // sum(weights)))
    least = 1 if total - largest >= number_of - 1 else 0
    given, surplus = [largest] + [least] * (number_of - 1), total - largest - least * (number_of - 1)
    while surplus > 0:
        free = [i for i in range(1, number_of) if given[i] < largest] or [i for i in range(1, number_of) if given[i] < bound]
        pool, budget = sum([weights[i] for i in free]), surplus
        for i in free:
            addition = min(bound - given[i], max(1, budget * weights[i] // pool), surplus)
            given[i] = given[i] + addition
            surplus = surplus - addition
    return np.array(given)


def normal_values(rng, dims, deviation, reach, split=(), kind=jnp.bfloat16):
    entries = deviation * jax.random.normal(rng, dims, jnp.float32)
    if split:
        entries = entries * shard_levels(rng, dims, split, -0.22, 0.18)
    return jnp.clip(entries, -reach, reach).astype(kind)


def setup_inputs(seed: int = 0) -> dict:
    key_of = jax.random.split(jax.random.key(seed), 8)
    patches = normal_values(key_of[0], (TOKENS, D), 1.0, 6.0, ((0, 32),))
    routes_keys = jax.random.split(jax.random.fold_in(key_of[1], 1), TOKENS // TOK_DEV)
    routes_turns = jax.random.permutation(jax.random.fold_in(key_of[1], 3), TOKENS // TOK_DEV)
    routes = jax.vmap(lambda own, number: routed_block(jax.random.fold_in(key_of[1], 2), own, number, TOK_DEV, EXPERTS, 2, CAP, 2))(routes_keys, routes_turns).reshape((TOKENS, 2))
    mix_weights = jnp.clip(0.25 + 0.75 * jax.random.uniform(key_of[2], (TOKENS, 2), jnp.float32) ** shard_levels(key_of[2], (TOKENS, 2), ((0, 32),), -0.2, 0.2), 0.25, 1.0)
    modulation = normal_values(key_of[3], (LATENTS, 3, D), 0.5, 3.0, (), jnp.float32)
    up_weight = normal_values(key_of[4], (EXPERTS * SPLIT, D, HIDDEN_SIZE // SPLIT), D ** -0.5, 0.125, ((0, 32),))
    down_weight = normal_values(key_of[5], (EXPERTS * SPLIT, HIDDEN_SIZE // SPLIT, D), HIDDEN_SIZE ** -0.5, 0.1875, ((0, 32),))
    cotangent = normal_values(key_of[6], (TOKENS, D), 1.0, 6.0, ((0, 32),))
    return {"patches": patches, "routes": routes, "mix_weights": mix_weights, "modulation": modulation, "up_weight": up_weight, "down_weight": down_weight, "cotangent": cotangent}


EPSILON = 1e-06

def modulate(inputs, offset, scaling):
    average = lax.optimization_barrier(jnp.mean(inputs, axis=-1, keepdims=True))
    centred = inputs - average
    spread = lax.optimization_barrier(jnp.mean(centred * centred, axis=-1, keepdims=True))
    normed = centred * lax.rsqrt(spread + EPSILON)
    return normed * (1.0 + scaling) + offset

def activate(hidden_pre):
    return jax.nn.gelu(hidden_pre, approximate=True)

def reference(patches, routes, mix_weights, modulation, up_weight, down_weight, cotangent):
    devices_all = N_SEQ * N_EXP
    tok_all = patches.shape[0]
    assign_count = 2 * tok_all
    offset = modulation[:, 0][:, None, :]
    scaling = modulation[:, 1][:, None, :]
    gating = modulation[:, 2][:, None, :]
    inputs = patches.astype(jnp.float32).reshape(LATENTS, -1, D)

    def shaped(rows_in):
        return modulate(rows_in, offset, scaling)
    modulated = shaped(inputs).astype(jnp.bfloat16).reshape(tok_all, D)
    grad_out = cotangent.astype(jnp.float32).reshape(LATENTS, -1, D)
    mix_latent = mix_weights.reshape(LATENTS, -1, 2)
    weighted = (mix_latent[..., None] * grad_out[:, :, None, :] * gating[:, :, None, :]).astype(jnp.bfloat16)
    weighted = weighted.reshape(assign_count, D)
    mod_pairs = jnp.repeat(modulated, 2, axis=0)
    zero_row = jnp.zeros((1, D), jnp.bfloat16)
    mod_extended = jnp.concatenate([mod_pairs, zero_row], axis=0)
    grad_extended = jnp.concatenate([weighted, zero_row], axis=0)
    flat_routes = routes.reshape(devices_all, -1)
    onehot = (flat_routes[:, :, None] == jnp.arange(EXPERTS, dtype=jnp.int32)[None, None, :]).astype(jnp.int32)
    before = jnp.cumsum(onehot, axis=1) - onehot
    position = lax.optimization_barrier(jnp.sum(before * onehot, axis=2)).astype(jnp.int32)
    block_ids = jnp.broadcast_to(jnp.arange(devices_all, dtype=jnp.int32)[:, None], flat_routes.shape)
    assign_ids = jnp.arange(assign_count, dtype=jnp.int32).reshape(devices_all, -1)
    slot_table = jnp.full((EXPERTS, devices_all, CAP), assign_count, jnp.int32)
    slot_table = slot_table.at[flat_routes, block_ids, position].set(assign_ids)

    def per_expert(expert_index):
        chosen = lax.dynamic_index_in_dim(slot_table, expert_index, 0, keepdims=False).reshape(-1)
        token_rows = mod_extended[chosen]
        grad_rows = grad_extended[chosen]
        part_total = jnp.zeros((token_rows.shape[0], D), jnp.float32)
        back_total = jnp.zeros((token_rows.shape[0], D), jnp.float32)
        grads_up = []
        grads_down = []
        for quarter in range(SPLIT):
            entry = expert_index * SPLIT + quarter
            up_local = lax.dynamic_index_in_dim(up_weight, entry, 0, keepdims=False)
            down_local = lax.dynamic_index_in_dim(down_weight, entry, 0, keepdims=False)
            hidden_pre = jnp.dot(token_rows, up_local, preferred_element_type=jnp.float32)
            activated = activate(hidden_pre).astype(jnp.bfloat16)
            partial_value = jnp.dot(activated, down_local, preferred_element_type=jnp.float32).astype(jnp.bfloat16)
            part_total = part_total + partial_value.astype(jnp.float32)
            grad_act = lax.dot_general(grad_rows, down_local, (((1,), (1,)), ((), ())), preferred_element_type=jnp.float32)
            grad_pre = jax.vjp(activate, hidden_pre)[1](grad_act)[0].astype(jnp.bfloat16)
            back_part = lax.dot_general(grad_pre, up_local, (((1,), (1,)), ((), ())), preferred_element_type=jnp.float32).astype(jnp.bfloat16)
            back_total = back_total + back_part.astype(jnp.float32)
            grads_down.append(lax.dot_general(activated, grad_rows, (((0,), (0,)), ((), ())), preferred_element_type=jnp.float32).astype(jnp.bfloat16))
            grads_up.append(lax.dot_general(token_rows, grad_pre, (((0,), (0,)), ((), ())), preferred_element_type=jnp.float32).astype(jnp.bfloat16))
        return (part_total.astype(jnp.bfloat16), back_total.astype(jnp.bfloat16), jnp.stack(grads_up), jnp.stack(grads_down))
    partials, backs, grads_up, grads_down = lax.map(per_expert, jnp.arange(EXPERTS, dtype=jnp.int32))
    flat_slots = slot_table.reshape(-1)
    out_pairs = jnp.zeros((assign_count + 1, D), jnp.float32).at[flat_slots].add(partials.reshape(-1, D).astype(jnp.float32))
    back_pairs = jnp.zeros((assign_count + 1, D), jnp.float32).at[flat_slots].add(backs.reshape(-1, D).astype(jnp.float32))
    out_pairs = out_pairs[:assign_count].reshape(LATENTS, -1, 2, D)
    back_pairs = back_pairs[:assign_count].reshape(LATENTS, -1, 2, D)
    moe = mix_latent[..., 0:1] * out_pairs[:, :, 0] + mix_latent[..., 1:2] * out_pairs[:, :, 1]
    mixed = (inputs + gating * moe).astype(jnp.bfloat16).reshape(tok_all, D)
    grad_mod = back_pairs[:, :, 0] + back_pairs[:, :, 1]
    grad_in = jax.vjp(shaped, inputs)[1](grad_mod)[0]
    grad_patches = (grad_out + grad_in).astype(jnp.bfloat16).reshape(tok_all, D)
    grad_up = grads_up.reshape(EXPERTS * SPLIT, D, -1)
    grad_down = grads_down.reshape(EXPERTS * SPLIT, -1, D)
    return (mixed, grad_patches, grad_up, grad_down)
```

```python
import math

import jax
import jax.numpy as jnp
from jax import lax
from jax.experimental import pallas as pl
from jax.experimental.pallas import tpu as pltpu
from jax.sharding import PartitionSpec as P

D = 2048
SPLIT = 4
LATENTS = 2

EPSILON = 1e-06
ROOT = math.sqrt(2.0 / math.pi)
CUBE = 0.044715
TILE = 256


def from_partner(value, axis, mask):
    pairs = [(source, source ^ mask) for source in range(lax.axis_size(axis))]
    return lax.ppermute(value, axis, pairs)


def from_group(value, axis, shift):
    count = lax.axis_size(axis)
    pairs = [(source, (source + shift) % count) for source in range(count)]
    return lax.ppermute(value, axis, pairs)


def modulate(inputs, offset, scaling):
    average = jnp.mean(inputs, axis=-1, keepdims=True)
    centred = inputs - average
    spread = jnp.mean(centred * centred, axis=-1, keepdims=True)
    normed = centred * lax.rsqrt(spread + EPSILON)
    return normed * (1.0 + scaling) + offset


def dot(a, b, dims):
    return lax.dot_general(a, b, ((dims[:1], dims[1:]), ((), ())), preferred_element_type=jnp.float32)


def forward_kernel(rows_ref, *refs):
    ups, downs = refs[:SPLIT], refs[SPLIT : 2 * SPLIT]
    hidden_ref, activated_ref, out_ref = refs[2 * SPLIT :]
    rows = rows_ref[...]
    for part in range(SPLIT):
        hidden = dot(rows, ups[part][...], (1, 0))
        hidden_ref[part] = hidden
        inner = jnp.tanh(ROOT * (hidden + CUBE * hidden * hidden * hidden))
        activated_ref[part] = (0.5 * hidden * (1.0 + inner)).astype(jnp.bfloat16)
    for start in range(0, out_ref.shape[1], TILE):
        cols = slice(start, start + TILE)
        total = dot(activated_ref[0], downs[0][:, cols], (1, 0))
        for part in range(1, SPLIT):
            total = total + dot(activated_ref[part], downs[part][:, cols], (1, 0))
        out_ref[:, cols] = total.astype(out_ref.dtype)


def backward_kernel(grad_ref, hidden_ref, activated_ref, *refs):
    ups, downs = refs[:SPLIT], refs[SPLIT : 2 * SPLIT]
    pre_ref, back_ref = refs[2 * SPLIT : 2 * SPLIT + 2]
    grad_downs = refs[2 * SPLIT + 2 :]
    grad = grad_ref[...]
    for part in range(SPLIT):
        grad_act = dot(grad, downs[part][...], (1, 1))
        hidden = hidden_ref[part]
        square = hidden * hidden
        inner = jnp.tanh(ROOT * (hidden + CUBE * square * hidden))
        slope = 0.5 * (1.0 + inner) + 0.5 * hidden * (1.0 - inner * inner) * (
            ROOT * (1.0 + 3.0 * CUBE * square)
        )
        pre_ref[part] = (grad_act * slope).astype(jnp.bfloat16)
    for start in range(0, back_ref.shape[1], TILE):
        cols = slice(start, start + TILE)
        total = dot(pre_ref[0], ups[0][cols, :], (1, 1))
        for part in range(1, SPLIT):
            total = total + dot(pre_ref[part], ups[part][cols, :], (1, 1))
        back_ref[:, cols] = total.astype(back_ref.dtype)
    for part in range(SPLIT):
        out = grad_downs[part]
        out[...] = dot(activated_ref[part], grad, (0, 0)).astype(out.dtype)


def grad_up_kernel(rows_ref, pre_ref, *grad_ups):
    rows = rows_ref[...]
    for part in range(SPLIT):
        out = grad_ups[part]
        out[...] = dot(rows, pre_ref[part], (0, 0)).astype(out.dtype)


def call(kernel, out_shape, *args):
    return pl.pallas_call(
        kernel,
        out_shape=out_shape,
        in_specs=[pl.BlockSpec(memory_space=pltpu.VMEM)] * len(args),
        out_specs=jax.tree.map(lambda _: pl.BlockSpec(memory_space=pltpu.VMEM), out_shape),
    )(*args)


def shards(patches, routes, mix_weights, modulation, up_weight, down_weight, cotangent):
    seq_count = lax.axis_size("seq")
    exp_count = lax.axis_size("exp")
    devices_all = seq_count * exp_count
    experts_all = devices_all // SPLIT
    groups = exp_count // SPLIT
    tok_rows, width = patches.shape
    hidden_size = up_weight.shape[-1]
    capacity = 2 * tok_rows // experts_all + max(1, tok_rows // (2 * experts_all))
    slot_count = seq_count * groups * capacity
    split_bits = SPLIT.bit_length() - 1
    my_group = lax.axis_index("exp") // SPLIT
    device_id = lax.axis_index("seq") * exp_count + lax.axis_index("exp")
    latent = LATENTS * device_id // devices_all
    params = lax.dynamic_index_in_dim(modulation, latent, 0, keepdims=False)
    offset, scaling, gating = params[0], params[1], params[2]
    inputs = patches.astype(jnp.float32)

    def shaped(rows_in):
        return modulate(rows_in, offset, scaling)

    def all_groups(value):
        return jnp.stack([value] + [from_group(value, "exp", k * SPLIT) for k in range(1, groups)])

    def holders(weight):
        parts = [weight]
        for bit in reversed(range(split_bits)):
            parts = parts + [from_partner(part, "exp", 1 << bit) for part in parts]
        return parts

    ups = holders(up_weight[0])
    downs = holders(down_weight[0])

    modulated = shaped(inputs).astype(jnp.bfloat16)
    mod_blocks = all_groups(modulated).reshape(groups * tok_rows, width)
    cot_blocks = all_groups(cotangent).reshape(groups * tok_rows, width)
    routes_all = all_groups(routes)
    mix_all = all_groups(mix_weights)

    expert_iota = lax.broadcasted_iota(jnp.int32, (1, 1, experts_all), 2)
    named = [(routes_all[:, :, k][:, :, None] == expert_iota).astype(jnp.bfloat16) for k in range(2)]
    both = named[0] + named[1]
    earlier = jnp.tri(tok_rows, tok_rows, -1, dtype=jnp.bfloat16)
    before = jnp.einsum("ts,gse->gte", earlier, both, preferred_element_type=jnp.float32)
    block_iota = lax.broadcasted_iota(jnp.int32, (groups, tok_rows), 0)
    slot_iota = lax.broadcasted_iota(jnp.int32, (slot_count, 1), 0)
    hits = []
    for k in range(2):
        position = jnp.sum(before * named[k].astype(jnp.float32), axis=2).astype(jnp.int32)
        expert = routes_all[:, :, k]
        slot = ((expert // groups) * groups + block_iota) * capacity + position
        slot = jnp.where(expert % groups == my_group, slot, -1).reshape(1, -1)
        hits.append(slot == slot_iota)
    placing = (hits[0] | hits[1]).astype(jnp.bfloat16)
    mixing = jnp.where(hits[0], mix_all[:, :, 0].reshape(1, -1), 0.0) + jnp.where(
        hits[1], mix_all[:, :, 1].reshape(1, -1), 0.0
    )
    mix_slot = jnp.sum(mixing, axis=1, keepdims=True)
    mix_high = mixing.astype(jnp.bfloat16)
    mix_low = (mixing - mix_high.astype(jnp.float32)).astype(jnp.bfloat16)

    def over_seq(rows):
        moved = lax.all_to_all(
            rows.reshape(seq_count, -1, width), "seq", split_axis=0, concat_axis=0, tiled=True
        )
        return moved.reshape(slot_count, width)

    def home(dense):
        dense = dense.reshape(groups, tok_rows, width)
        total = dense[0]
        for k in range(1, groups):
            returned = from_group(dense[k].astype(jnp.bfloat16), "exp", -k * SPLIT)
            total = total + returned.astype(jnp.float32)
        return total

    token_rows = over_seq(dot(placing, mod_blocks, (1, 0)).astype(jnp.bfloat16))
    weighted = (mix_slot * dot(placing, cot_blocks, (1, 0))) * gating
    grad_rows = over_seq(weighted.astype(jnp.bfloat16))

    rows_bf16 = jax.ShapeDtypeStruct((slot_count, width), jnp.bfloat16)
    hid = (SPLIT, slot_count, hidden_size)
    half = SPLIT // 2
    kinds = [jnp.float32] * half + [jnp.bfloat16] * half
    hidden_pre, activated, out_rows = call(
        forward_kernel,
        (jax.ShapeDtypeStruct(hid, jnp.float32), jax.ShapeDtypeStruct(hid, jnp.bfloat16), rows_bf16),
        token_rows,
        *ups,
        *downs,
    )
    grad_pre, back_rows, *grad_downs = call(
        backward_kernel,
        (
            jax.ShapeDtypeStruct(hid, jnp.bfloat16),
            rows_bf16,
            *[jax.ShapeDtypeStruct((hidden_size, width), kind) for kind in kinds],
        ),
        grad_rows,
        hidden_pre,
        activated,
        *ups,
        *downs,
    )
    grad_ups = call(
        grad_up_kernel,
        tuple(jax.ShapeDtypeStruct((width, hidden_size), kind) for kind in kinds),
        token_rows,
        grad_pre,
    )

    def to_holder(parts):
        parts = list(parts)
        for bit in range(split_bits):
            count = len(parts) // 2
            given = [from_partner(p.astype(jnp.bfloat16), "exp", 1 << bit) for p in parts[count:]]
            parts = [mine + other.astype(jnp.float32) for mine, other in zip(parts, given)]
        return parts[0].astype(jnp.bfloat16)[None]

    out_back = over_seq(out_rows)
    moe = home(dot(mix_high, out_back, (0, 0)) + dot(mix_low, out_back, (0, 0)))
    back_back = over_seq(back_rows)
    grad_mod = home(dot(placing, back_back, (0, 0)))
    grad_down = to_holder(grad_downs)
    grad_up = to_holder(grad_ups)

    mixed = (inputs + gating * moe).astype(jnp.bfloat16)
    grad_in = jax.vjp(shaped, inputs)[1](grad_mod)[0]
    grad_patches = (cotangent.astype(jnp.float32) + grad_in).astype(jnp.bfloat16)
    return (mixed, grad_patches, grad_up, grad_down)


def solution(mesh):
    return jax.shard_map(
        shards,
        mesh=mesh,
        in_specs=(
            P(("seq", "exp"), None),
            P(("seq", "exp"), None),
            P(("seq", "exp"), None),
            P(),
            P(("seq", "exp"), None, None),
            P(("seq", "exp"), None, None),
            P(("seq", "exp"), None),
        ),
        out_specs=(
            P(("seq", "exp"), None),
            P(("seq", "exp"), None),
            P(("seq", "exp"), None, None),
            P(("seq", "exp"), None, None),
        ),
        check_vma=False,
    )
```

```python
import math

import jax
import jax.numpy as jnp
from jax import lax
from jax.experimental import pallas as pl
from jax.experimental.pallas import tpu as pltpu
from jax.sharding import PartitionSpec as P

D = 2048
SPLIT = 4
LATENTS = 2

EPSILON = 1e-06
ROOT = math.sqrt(2.0 / math.pi)
CUBE = 0.044715
TILE = 256


def from_partner(value, axis, mask):
    pairs = [(source, source ^ mask) for source in range(lax.axis_size(axis))]
    return lax.ppermute(value, axis, pairs)


def from_group(value, axis, shift):
    count = lax.axis_size(axis)
    pairs = [(source, (source + shift) % count) for source in range(count)]
    return lax.ppermute(value, axis, pairs)


def modulate(inputs, offset, scaling):
    average = jnp.mean(inputs, axis=-1, keepdims=True)
    centred = inputs - average
    spread = jnp.mean(centred * centred, axis=-1, keepdims=True)
    normed = centred * lax.rsqrt(spread + EPSILON)
    return normed * (1.0 + scaling) + offset


def dot(a, b, dims):
    return lax.dot_general(a, b, ((dims[:1], dims[1:]), ((), ())), preferred_element_type=jnp.float32)


def gelu_slope(hidden):
    square = hidden * hidden
    inner = jnp.tanh(ROOT * (hidden + CUBE * square * hidden))
    return 0.5 * (1.0 + inner) + 0.5 * hidden * (1.0 - inner * inner) * (
        ROOT * (1.0 + 3.0 * CUBE * square)
    )


def modulate_kernel(patches_ref, params_ref, out_ref):
    inputs = patches_ref[...].astype(jnp.float32)
    out_ref[...] = modulate(inputs, params_ref[0:1], params_ref[1:2]).astype(out_ref.dtype)


def chunk_hits(slots, relative, capacity):
    rows = relative * capacity + lax.broadcasted_iota(jnp.int32, (capacity, 1), 0)
    return slots[0:1] == rows, slots[1:2] == rows


def place_kernel(slots_ref, block_ref, *outs):
    slots, block = slots_ref[...], block_ref[...]
    for relative, out in enumerate(outs):
        first, second = chunk_hits(slots, relative, out.shape[0])
        placing = jnp.where(first | second, 1.0, 0.0).astype(jnp.bfloat16)
        out[...] = dot(placing, block, (1, 0)).astype(out.dtype)


def place_weighted_kernel(slots_ref, mix_ref, params_ref, block_ref, *outs):
    slots, mix, block, gating = slots_ref[...], mix_ref[...], block_ref[...], params_ref[2:3]
    for relative, out in enumerate(outs):
        first, second = chunk_hits(slots, relative, out.shape[0])
        placing = jnp.where(first | second, 1.0, 0.0).astype(jnp.bfloat16)
        mixing = jnp.where(first, mix[0:1], 0.0) + jnp.where(second, mix[1:2], 0.0)
        scale = jnp.sum(mixing, axis=1, keepdims=True)
        out[...] = ((scale * dot(placing, block, (1, 0))) * gating).astype(out.dtype)


def gathered(slots, mix, chunks):
    total = None
    for relative, chunk in enumerate(chunks):
        capacity = chunk.shape[0]
        columns = relative * capacity + lax.broadcasted_iota(jnp.int32, (1, capacity), 1)
        first, second = slots[:, 0:1] == columns, slots[:, 1:2] == columns
        rows = chunk[...]
        if mix is None:
            weights = [jnp.where(first | second, 1.0, 0.0).astype(jnp.bfloat16)]
        else:
            mixing = jnp.where(first, mix[:, 0:1], 0.0) + jnp.where(second, mix[:, 1:2], 0.0)
            high = mixing.astype(jnp.bfloat16)
            weights = [high, (mixing - high.astype(jnp.float32)).astype(jnp.bfloat16)]
        for weight in weights:
            value = dot(weight, rows, (1, 0))
            total = value if total is None else total + value
    return total


def combine_kernel(slots_ref, *refs):
    out = refs[-1]
    out[...] = gathered(slots_ref[...], None, refs[:-1]).astype(out.dtype)


def combine_mixed_kernel(slots_ref, mix_ref, *refs):
    out = refs[-1]
    out[...] = gathered(slots_ref[...], mix_ref[...], refs[:-1]).astype(out.dtype)


def finish_mixed_kernel(count, slots_ref, mix_ref, patches_ref, params_ref, *refs):
    out = refs[-1]
    moe = gathered(slots_ref[...], mix_ref[...], refs[:count])
    for other in refs[count:-1]:
        moe = moe + other[...].astype(jnp.float32)
    out[...] = (patches_ref[...].astype(jnp.float32) + params_ref[2:3] * moe).astype(out.dtype)


def finish_grad_kernel(count, slots_ref, patches_ref, params_ref, cotangent_ref, *refs):
    out = refs[-1]
    grad = gathered(slots_ref[...], None, refs[:count])
    for other in refs[count:-1]:
        grad = grad + other[...].astype(jnp.float32)
    inputs = patches_ref[...].astype(jnp.float32)
    centred = inputs - jnp.mean(inputs, axis=-1, keepdims=True)
    inverse = lax.rsqrt(jnp.mean(centred * centred, axis=-1, keepdims=True) + EPSILON)
    normed = centred * inverse
    scaled = grad * (1.0 + params_ref[1:2])
    along = jnp.mean(scaled * normed, axis=-1, keepdims=True)
    level = jnp.mean(scaled, axis=-1, keepdims=True)
    grad_in = inverse * (scaled - level - normed * along)
    out[...] = (cotangent_ref[...].astype(jnp.float32) + grad_in).astype(out.dtype)


def hidden_kernel(rows_ref, *refs):
    ups, (hidden_ref, activated_ref) = refs[:SPLIT], refs[SPLIT:]
    rows = rows_ref[...]
    for part in range(SPLIT):
        hidden = dot(rows, ups[part][...], (1, 0))
        hidden_ref[part] = hidden
        inner = jnp.tanh(ROOT * (hidden + CUBE * hidden * hidden * hidden))
        activated_ref[part] = (0.5 * hidden * (1.0 + inner)).astype(jnp.bfloat16)


def grad_down_kernel(activated_ref, grad_ref, *outs):
    grad = grad_ref[...]
    for part, out in enumerate(outs):
        out[...] = dot(activated_ref[part], grad, (0, 0)).astype(out.dtype)


def grad_up_kernel(rows_ref, pre_ref, *outs):
    rows = rows_ref[...]
    for part, out in enumerate(outs):
        out[...] = dot(rows, pre_ref[part], (0, 0)).astype(out.dtype)


def store_chunks(outs, cols, total):
    capacity = outs[0].shape[0]
    for number, out in enumerate(outs):
        out[:, cols] = total[number * capacity : (number + 1) * capacity].astype(out.dtype)


def out_kernel(activated_ref, *refs):
    downs, outs = refs[:SPLIT], refs[SPLIT:]
    for start in range(0, outs[0].shape[1], TILE):
        cols = slice(start, start + TILE)
        total = dot(activated_ref[0], downs[0][:, cols], (1, 0))
        for part in range(1, SPLIT):
            total = total + dot(activated_ref[part], downs[part][:, cols], (1, 0))
        store_chunks(outs, cols, total)


def backward_kernel(grad_ref, hidden_ref, *refs):
    ups, downs, pre_ref, outs = refs[:SPLIT], refs[SPLIT : 2 * SPLIT], refs[2 * SPLIT], refs[2 * SPLIT + 1 :]
    grad = grad_ref[...]
    for part in range(SPLIT):
        grad_act = dot(grad, downs[part][...], (1, 1))
        pre_ref[part] = (grad_act * gelu_slope(hidden_ref[part])).astype(jnp.bfloat16)
    for start in range(0, outs[0].shape[1], TILE):
        cols = slice(start, start + TILE)
        total = dot(pre_ref[0], ups[0][cols, :], (1, 1))
        for part in range(1, SPLIT):
            total = total + dot(pre_ref[part], ups[part][cols, :], (1, 1))
        store_chunks(outs, cols, total)


def call(kernel, out_shape, *args):
    return pl.pallas_call(
        kernel,
        out_shape=out_shape,
        in_specs=[pl.BlockSpec(memory_space=pltpu.VMEM)] * len(args),
        out_specs=jax.tree.map(lambda _: pl.BlockSpec(memory_space=pltpu.VMEM), out_shape),
    )(*args)


def shards(patches, routes, mix_weights, modulation, up_weight, down_weight, cotangent):
    seq_count = lax.axis_size("seq")
    exp_count = lax.axis_size("exp")
    devices_all = seq_count * exp_count
    experts_all = devices_all // SPLIT
    groups = exp_count // SPLIT
    tok_rows, width = patches.shape
    hidden_size = up_weight.shape[-1]
    capacity = 2 * tok_rows // experts_all + max(1, tok_rows // (2 * experts_all))
    slot_count = seq_count * groups * capacity
    split_bits = SPLIT.bit_length() - 1
    my_group = lax.axis_index("exp") // SPLIT
    my_column = lax.axis_index("seq")
    device_id = my_column * exp_count + lax.axis_index("exp")
    latent = LATENTS * device_id // devices_all
    params = lax.dynamic_index_in_dim(modulation, latent, 0, keepdims=False)

    def shape(dims, kind=jnp.bfloat16):
        return jax.ShapeDtypeStruct(dims, kind)

    def all_groups(value):
        return [value] + [from_group(value, "exp", k * SPLIT) for k in range(1, groups)]

    def holders(weight):
        parts = [weight]
        for bit in reversed(range(split_bits)):
            parts = parts + [from_partner(part, "exp", 1 << bit) for part in parts]
        return parts

    meta = jnp.concatenate([routes.astype(jnp.float32), mix_weights], axis=1).T
    with jax.named_scope("meta"):
        metas = all_groups(meta)
    with jax.named_scope("upw"):
        ups = holders(up_weight[0])
    with jax.named_scope("mod"):
        modulated = call(modulate_kernel, shape((tok_rows, width)), patches, params)
        mods = all_groups(modulated)
    with jax.named_scope("cot"):
        cots = all_groups(cotangent)
    with jax.named_scope("downw"):
        downs = holders(down_weight[0])

    def tables(block_meta):
        expert = block_meta[:2].astype(jnp.int32)
        expert_iota = lax.broadcasted_iota(jnp.int32, (experts_all, tok_rows), 0)
        named = [(expert[k : k + 1] == expert_iota).astype(jnp.float32) for k in range(2)]
        earlier = jnp.tri(tok_rows, tok_rows, -1, dtype=jnp.bfloat16)
        before = lax.dot_general(
            (named[0] + named[1]).astype(jnp.bfloat16),
            earlier,
            (((1,), (1,)), ((), ())),
            preferred_element_type=jnp.float32,
        )
        position = jnp.stack([jnp.sum(before * named[k], axis=0) for k in range(2)]).astype(jnp.int32)
        relative = (expert // groups) ^ my_column
        slots = jnp.where(expert % groups == my_group, relative * capacity + position, -1)
        mix = block_meta[2:]
        return slots, mix, slots.T, mix.T

    info = [tables(block_meta) for block_meta in metas]

    def exchange(chunks):
        return [chunks[0]] + [from_partner(chunks[r], "seq", r) for r in range(1, seq_count)]

    chunk_shapes = (shape((capacity, width)),) * seq_count
    token_chunks, grad_chunks = [], []
    for b in range(groups):
        with jax.named_scope(f"tok{b}"):
            token_chunks += exchange(call(place_kernel, chunk_shapes, info[b][0], mods[b]))
    for b in range(groups):
        with jax.named_scope(f"grd{b}"):
            grad_chunks += exchange(
                call(place_weighted_kernel, chunk_shapes, info[b][0], info[b][1], params, cots[b])
            )
    token_rows = jnp.concatenate(token_chunks, axis=0)
    grad_rows = jnp.concatenate(grad_chunks, axis=0)

    hid = (SPLIT, slot_count, hidden_size)
    half = SPLIT // 2
    kinds = [jnp.float32] * half + [jnp.bfloat16] * half
    all_chunks = chunk_shapes * groups

    def to_holder(parts):
        parts = list(parts)
        for bit in range(split_bits):
            count = len(parts) // 2
            given = [from_partner(p.astype(jnp.bfloat16), "exp", 1 << bit) for p in parts[count:]]
            parts = [mine + other.astype(jnp.float32) for mine, other in zip(parts, given)]
        return parts[0].astype(jnp.bfloat16)[None]

    hidden_pre, activated = call(
        hidden_kernel, (shape(hid, jnp.float32), shape(hid)), token_rows, *ups
    )
    grad_downs = call(
        grad_down_kernel,
        tuple(shape((hidden_size, width), kind) for kind in kinds),
        activated,
        grad_rows,
    )
    with jax.named_scope("gdown"):
        grad_down = to_holder(grad_downs)
    out_chunks = call(out_kernel, all_chunks, activated, *downs)
    grad_pre, *back_chunks = call(
        backward_kernel, (shape(hid), *all_chunks), grad_rows, hidden_pre, *ups, *downs
    )
    grad_ups = call(
        grad_up_kernel,
        tuple(shape((width, hidden_size), kind) for kind in kinds),
        token_rows,
        grad_pre,
    )
    with jax.named_scope("gup"):
        grad_up = to_holder(grad_ups)

    def returned(chunks, combine, scope):
        blocks = [list(chunks[b * seq_count : (b + 1) * seq_count]) for b in range(groups)]
        homes = []
        for b in range(1, groups):
            with jax.named_scope(scope + "far"):
                arrived = exchange(blocks[b])
            with jax.named_scope(scope + "home"):
                homes.append(from_group(combine(b, arrived), "exp", -b * SPLIT))
        with jax.named_scope(scope + "near"):
            return exchange(blocks[0]), homes

    dense = shape((tok_rows, width))
    near, homes = returned(
        out_chunks,
        lambda b, arrived: call(combine_mixed_kernel, dense, info[b][2], info[b][3], *arrived),
        "out",
    )
    mixed = call(
        lambda *refs: finish_mixed_kernel(seq_count, *refs),
        dense,
        info[0][2],
        info[0][3],
        patches,
        params,
        *near,
        *homes,
    )
    near, homes = returned(
        back_chunks, lambda b, arrived: call(combine_kernel, dense, info[b][2], *arrived), "back"
    )
    grad_patches = call(
        lambda *refs: finish_grad_kernel(seq_count, *refs),
        dense,
        info[0][2],
        patches,
        params,
        cotangent,
        *near,
        *homes,
    )
    return (mixed, grad_patches, grad_up, grad_down)


def solution(mesh):
    return jax.shard_map(
        shards,
        mesh=mesh,
        in_specs=(
            P(("seq", "exp"), None),
            P(("seq", "exp"), None),
            P(("seq", "exp"), None),
            P(),
            P(("seq", "exp"), None, None),
            P(("seq", "exp"), None, None),
            P(("seq", "exp"), None),
        ),
        out_specs=(
            P(("seq", "exp"), None),
            P(("seq", "exp"), None),
            P(("seq", "exp"), None, None),
            P(("seq", "exp"), None, None),
        ),
        check_vma=False,
    )
```

```python
import math

import jax
import jax.numpy as jnp
from jax import lax
from jax.experimental import pallas as pl
from jax.experimental.pallas import tpu as pltpu
from jax.sharding import PartitionSpec as P


SPLIT = 4
LATENTS = 2

EPSILON = 1e-06
ROOT = math.sqrt(2.0 / math.pi)
CUBE = 0.044715
TILE = 256


def from_partner(value, axis, mask):
    pairs = [(source, source ^ mask) for source in range(lax.axis_size(axis))]
    return lax.ppermute(value, axis, pairs)


def from_group(value, axis, shift):
    count = lax.axis_size(axis)
    pairs = [(source, (source + shift) % count) for source in range(count)]
    return lax.ppermute(value, axis, pairs)


def modulate(inputs, offset, scaling):
    average = jnp.mean(inputs, axis=-1, keepdims=True)
    centred = inputs - average
    spread = jnp.mean(centred * centred, axis=-1, keepdims=True)
    normed = centred * lax.rsqrt(spread + EPSILON)
    return normed * (1.0 + scaling) + offset


def dot(a, b, dims):
    return lax.dot_general(a, b, ((dims[:1], dims[1:]), ((), ())), preferred_element_type=jnp.float32)


def gelu_slope(hidden):
    square = hidden * hidden
    inner = jnp.tanh(ROOT * (hidden + CUBE * square * hidden))
    return 0.5 * (1.0 + inner) + 0.5 * hidden * (1.0 - inner * inner) * (
        ROOT * (1.0 + 3.0 * CUBE * square)
    )


def modulate_kernel(latent_ref, patches_ref, modulation_ref, out_ref):
    inputs = patches_ref[...].astype(jnp.float32)
    params = modulation_ref[latent_ref[0]]
    out_ref[...] = modulate(inputs, params[0:1], params[1:2]).astype(out_ref.dtype)


def chunk_hits(slots, relative, capacity):
    rows = relative * capacity + lax.broadcasted_iota(jnp.int32, (capacity, 1), 0)
    return slots[0:1] == rows, slots[1:2] == rows


def place_kernel(slots_ref, block_ref, *outs):
    slots, block = slots_ref[...], block_ref[...]
    for relative, out in enumerate(outs):
        first, second = chunk_hits(slots, relative, out.shape[0])
        placing = jnp.where(first | second, 1.0, 0.0).astype(jnp.bfloat16)
        out[...] = dot(placing, block, (1, 0)).astype(out.dtype)


def place_weighted_kernel(slots_ref, mix_ref, params_ref, block_ref, *outs):
    slots, mix, block, gating = slots_ref[...], mix_ref[...], block_ref[...], params_ref[2:3]
    for relative, out in enumerate(outs):
        first, second = chunk_hits(slots, relative, out.shape[0])
        placing = jnp.where(first | second, 1.0, 0.0).astype(jnp.bfloat16)
        mixing = jnp.where(first, mix[0:1], 0.0) + jnp.where(second, mix[1:2], 0.0)
        scale = jnp.sum(mixing, axis=1, keepdims=True)
        out[...] = ((scale * dot(placing, block, (1, 0))) * gating).astype(out.dtype)


def gathered(slots, mix, chunks):
    total = None
    for relative, chunk in enumerate(chunks):
        capacity = chunk.shape[0]
        columns = relative * capacity + lax.broadcasted_iota(jnp.int32, (1, capacity), 1)
        first, second = slots[:, 0:1] == columns, slots[:, 1:2] == columns
        rows = chunk[...]
        if mix is None:
            weights = [jnp.where(first | second, 1.0, 0.0).astype(jnp.bfloat16)]
        else:
            mixing = jnp.where(first, mix[:, 0:1], 0.0) + jnp.where(second, mix[:, 1:2], 0.0)
            high = mixing.astype(jnp.bfloat16)
            weights = [high, (mixing - high.astype(jnp.float32)).astype(jnp.bfloat16)]
        for weight in weights:
            value = dot(weight, rows, (1, 0))
            total = value if total is None else total + value
    return total


def combine_kernel(slots_ref, *refs):
    out = refs[-1]
    out[...] = gathered(slots_ref[...], None, refs[:-1]).astype(out.dtype)


def combine_mixed_kernel(slots_ref, mix_ref, *refs):
    out = refs[-1]
    out[...] = gathered(slots_ref[...], mix_ref[...], refs[:-1]).astype(out.dtype)


def finish_mixed_kernel(count, slots_ref, mix_ref, patches_ref, params_ref, *refs):
    out = refs[-1]
    moe = gathered(slots_ref[...], mix_ref[...], refs[:count])
    for other in refs[count:-1]:
        moe = moe + other[...].astype(jnp.float32)
    out[...] = (patches_ref[...].astype(jnp.float32) + params_ref[2:3] * moe).astype(out.dtype)


def finish_grad_kernel(count, slots_ref, patches_ref, params_ref, cotangent_ref, *refs):
    out = refs[-1]
    grad = gathered(slots_ref[...], None, refs[:count])
    for other in refs[count:-1]:
        grad = grad + other[...].astype(jnp.float32)
    inputs = patches_ref[...].astype(jnp.float32)
    centred = inputs - jnp.mean(inputs, axis=-1, keepdims=True)
    inverse = lax.rsqrt(jnp.mean(centred * centred, axis=-1, keepdims=True) + EPSILON)
    normed = centred * inverse
    scaled = grad * (1.0 + params_ref[1:2])
    along = jnp.mean(scaled * normed, axis=-1, keepdims=True)
    level = jnp.mean(scaled, axis=-1, keepdims=True)
    grad_in = inverse * (scaled - level - normed * along)
    out[...] = (cotangent_ref[...].astype(jnp.float32) + grad_in).astype(out.dtype)


def hidden_kernel(rows_ref, *refs):
    ups, (hidden_ref, activated_ref) = refs[:SPLIT], refs[SPLIT:]
    rows = rows_ref[...]
    for part in range(SPLIT):
        hidden = dot(rows, ups[part][...], (1, 0))
        hidden_ref[part] = hidden
        inner = jnp.tanh(ROOT * (hidden + CUBE * hidden * hidden * hidden))
        activated_ref[part] = (0.5 * hidden * (1.0 + inner)).astype(jnp.bfloat16)


def grad_down_kernel(activated_ref, grad_ref, *outs):
    grad = grad_ref[...]
    for part, out in enumerate(outs):
        out[...] = dot(activated_ref[part], grad, (0, 0)).astype(out.dtype)


def grad_up_kernel(rows_ref, pre_ref, *outs):
    rows = rows_ref[...]
    for part, out in enumerate(outs):
        out[...] = dot(rows, pre_ref[part], (0, 0)).astype(out.dtype)


def store_chunks(outs, cols, total):
    capacity = outs[0].shape[0]
    for number, out in enumerate(outs):
        out[:, cols] = total[number * capacity : (number + 1) * capacity].astype(out.dtype)


def out_kernel(activated_ref, *refs):
    downs, outs = refs[:SPLIT], refs[SPLIT:]
    for start in range(0, outs[0].shape[1], TILE):
        cols = slice(start, start + TILE)
        total = dot(activated_ref[0], downs[0][:, cols], (1, 0))
        for part in range(1, SPLIT):
            total = total + dot(activated_ref[part], downs[part][:, cols], (1, 0))
        store_chunks(outs, cols, total)


def backward_kernel(grad_ref, hidden_ref, *refs):
    ups, downs, pre_ref, outs = refs[:SPLIT], refs[SPLIT : 2 * SPLIT], refs[2 * SPLIT], refs[2 * SPLIT + 1 :]
    grad = grad_ref[...]
    for part in range(SPLIT):
        grad_act = dot(grad, downs[part][...], (1, 1))
        pre_ref[part] = (grad_act * gelu_slope(hidden_ref[part])).astype(jnp.bfloat16)
    for start in range(0, outs[0].shape[1], TILE):
        cols = slice(start, start + TILE)
        total = dot(pre_ref[0], ups[0][cols, :], (1, 1))
        for part in range(1, SPLIT):
            total = total + dot(pre_ref[part], ups[part][cols, :], (1, 1))
        store_chunks(outs, cols, total)


def call(kernel, out_shape, *args, flops=0):
    cost = None
    if flops:
        cost = pl.CostEstimate(flops=flops, transcendentals=0, bytes_accessed=flops // 256)
    return pl.pallas_call(
        kernel,
        cost_estimate=cost,
        out_shape=out_shape,
        in_specs=[pl.BlockSpec(memory_space=pltpu.VMEM)] * len(args),
        out_specs=jax.tree.map(lambda _: pl.BlockSpec(memory_space=pltpu.VMEM), out_shape),
    )(*args)


def shards(patches, routes, mix_weights, modulation, up_weight, down_weight, cotangent):
    seq_count = lax.axis_size("seq")
    exp_count = lax.axis_size("exp")
    devices_all = seq_count * exp_count
    experts_all = devices_all // SPLIT
    groups = exp_count // SPLIT
    tok_rows, width = patches.shape
    hidden_size = up_weight.shape[-1]
    capacity = 2 * tok_rows // experts_all + max(1, tok_rows // (2 * experts_all))
    slot_count = seq_count * groups * capacity
    split_bits = SPLIT.bit_length() - 1
    my_group = lax.axis_index("exp") // SPLIT
    my_column = lax.axis_index("seq")
    device_id = my_column * exp_count + lax.axis_index("exp")
    latent = LATENTS * device_id // devices_all
    params = lax.dynamic_index_in_dim(modulation, latent, 0, keepdims=False)

    def shape(dims, kind=jnp.bfloat16):
        return jax.ShapeDtypeStruct(dims, kind)

    def all_groups(value):
        return [value] + [from_group(value, "exp", k * SPLIT) for k in range(1, groups)]

    def holders(weight):
        parts = [weight]
        for bit in reversed(range(split_bits)):
            parts = parts + [from_partner(part, "exp", 1 << bit) for part in parts]
        return parts

    meta = jnp.concatenate([routes.T.astype(jnp.float32), mix_weights.T], axis=0)
    metas = all_groups(meta)
    cots = all_groups(cotangent)
    modulated = pl.pallas_call(
        modulate_kernel,
        out_shape=shape((tok_rows, width)),
        in_specs=[pl.BlockSpec(memory_space=pltpu.SMEM)]
        + [pl.BlockSpec(memory_space=pltpu.VMEM)] * 2,
        out_specs=pl.BlockSpec(memory_space=pltpu.VMEM),
    )(latent.reshape(1).astype(jnp.int32), patches, modulation)
    mods = all_groups(modulated)
    ups = holders(up_weight[0])
    downs = holders(down_weight[0])

    def tables(block_meta):
        expert = block_meta[:2].astype(jnp.int32)
        expert_iota = lax.broadcasted_iota(jnp.int32, (experts_all, tok_rows), 0)
        named = [(expert[k : k + 1] == expert_iota).astype(jnp.float32) for k in range(2)]
        earlier = jnp.tri(tok_rows, tok_rows, -1, dtype=jnp.bfloat16)
        before = lax.dot_general(
            (named[0] + named[1]).astype(jnp.bfloat16),
            earlier,
            (((1,), (1,)), ((), ())),
            preferred_element_type=jnp.float32,
        )
        position = jnp.stack([jnp.sum(before * named[k], axis=0) for k in range(2)]).astype(jnp.int32)
        relative = (expert // groups) ^ my_column
        slots = jnp.where(expert % groups == my_group, relative * capacity + position, -1)
        mix = block_meta[2:]
        return slots, mix, slots.T, mix.T

    my_meta, _ = lax.optimization_barrier((metas[0], modulated))
    info = [tables(block_meta) for block_meta in [my_meta] + metas[1:]]

    def exchange(chunks):
        return [chunks[0]] + [from_partner(chunks[r], "seq", r) for r in range(1, seq_count)]

    chunk_shapes = (shape((capacity, width)),) * seq_count
    token_chunks, grad_chunks = [], []
    for b in range(groups):
        placed = call(place_kernel, chunk_shapes, info[b][0], mods[b])
        token_chunks += exchange(placed)
    for b in range(groups):
        grad_chunks += exchange(
            call(place_weighted_kernel, chunk_shapes, info[b][0], info[b][1], params, cots[b])
        )
    token_rows = jnp.concatenate(token_chunks, axis=0)
    grad_rows = jnp.concatenate(grad_chunks, axis=0)

    hid = (SPLIT, slot_count, hidden_size)
    half = SPLIT // 2
    kinds = [jnp.float32] * half + [jnp.bfloat16] * half
    all_chunks = chunk_shapes * groups

    def to_holder(parts):
        parts = list(parts)
        for bit in range(split_bits):
            count = len(parts) // 2
            given = [from_partner(p.astype(jnp.bfloat16), "exp", 1 << bit) for p in parts[count:]]
            parts = [mine + other.astype(jnp.float32) for mine, other in zip(parts, given)]
        return parts[0].astype(jnp.bfloat16)[None]

    work = 2 * slot_count * width * SPLIT * hidden_size
    hidden_pre, activated = call(
        hidden_kernel, (shape(hid, jnp.float32), shape(hid)), token_rows, *ups, flops=work
    )
    grad_downs = call(
        grad_down_kernel,
        tuple(shape((hidden_size, width), kind) for kind in kinds),
        activated,
        grad_rows,
        flops=work,
    )
    activated, grad_downs = lax.optimization_barrier((activated, grad_downs))
    grad_down = to_holder(grad_downs)
    out_chunks = call(out_kernel, all_chunks, activated, *downs, flops=work)
    hidden_pre, out_chunks = lax.optimization_barrier((hidden_pre, out_chunks))
    grad_pre, *back_chunks = call(
        backward_kernel,
        (shape(hid), *all_chunks),
        grad_rows,
        hidden_pre,
        *ups,
        *downs,
        flops=2 * work,
    )
    grad_ups = call(
        grad_up_kernel,
        tuple(shape((width, hidden_size), kind) for kind in kinds),
        token_rows,
        grad_pre,
        flops=work,
    )
    grad_up = to_holder(grad_ups)

    def returned(chunks, combine):
        blocks = [list(chunks[b * seq_count : (b + 1) * seq_count]) for b in range(groups)]
        homes = []
        for b in range(1, groups):
            arrived = exchange(blocks[b])
            dense_rows = combine(b, arrived)
            homes.append(from_group(dense_rows, "exp", -b * SPLIT))
        return exchange(blocks[0]), homes

    dense = shape((tok_rows, width))
    near, homes = returned(
        out_chunks,
        lambda b, arrived: call(combine_mixed_kernel, dense, info[b][2], info[b][3], *arrived),
    )
    mixed = call(
        lambda *refs: finish_mixed_kernel(seq_count, *refs),
        dense,
        info[0][2],
        info[0][3],
        patches,
        params,
        *near,
        *homes,
    )
    near, homes = returned(
        back_chunks, lambda b, arrived: call(combine_kernel, dense, info[b][2], *arrived)
    )
    grad_patches = call(
        lambda *refs: finish_grad_kernel(seq_count, *refs),
        dense,
        info[0][2],
        patches,
        params,
        cotangent,
        *near,
        *homes,
    )
    return (mixed, grad_patches, grad_up, grad_down)


def solution(mesh):
    return jax.shard_map(
        shards,
        mesh=mesh,
        in_specs=(
            P(("seq", "exp"), None),
            P(("seq", "exp"), None),
            P(("seq", "exp"), None),
            P(),
            P(("seq", "exp"), None, None),
            P(("seq", "exp"), None, None),
            P(("seq", "exp"), None),
        ),
        out_specs=(
            P(("seq", "exp"), None),
            P(("seq", "exp"), None),
            P(("seq", "exp"), None, None),
            P(("seq", "exp"), None, None),
        ),
        check_vma=False,
    )
```
